256 devices in a mesh: groups: 2 (over z), adapter: 16 (over x, core), tensor: 8 (over y).
Axes of the slice: x: 8, y: 8, z: 2, core: 2. Of those that a mesh axis runs over, the one named last changes fastest.
The devices are a block of a 8x8x16 slice.
Arguments:
- tokens: bfloat16 [8192, 8192], P(('groups', 'adapter'), 'tensor'), parts along dimension 0, may hold values from -6 to 6
- query_weight: bfloat16 [8192, 8192], P('tensor', 'adapter'), may hold values from -0.0625 to 0.0625
- adapter_down_weight: bfloat16 [512, 16, 8192], P('adapter', None, 'tensor'), may hold values from -0.0625 to 0.0625
- adapter_up_weight: bfloat16 [512, 16, 8192], P('adapter'), may hold values from -1.5 to 1.5
- block_adapter_ids: int32 [64], P('groups'), parts along dimension 0, may hold values from 0 to 511, as said below
- block_live_count: int32 [64], P('groups'), parts along dimension 0, may hold values from 1 to 128
- adapter_slot_index: int32 [1024], P('groups'), parts along dimension 0, may hold values from 0 to 511, as said below
Outputs:
- query: bfloat16 [8192, 8192], P(('groups', 'tensor'), 'adapter'), parts along dimension 0
The draws below stay inside these ranges and needn't reach their ends.
There are 2 independent parts, one for each index of `groups`. The reference program is written for one: setup_inputs(seed, part) draws one part's arguments, and reference() takes and returns one part's arrays. A program takes and returns all parts, laid end to end along the dimension named above; an argument that names none is the same for every part. Nothing has to cross between parts.
Inputs may be any that keep to these rules, and one draw needn't show every extreme that they name: Counting blocks by the owner range adapter_slot_index[block_adapter_ids[k]] // 32, no owner has more than 4 blocks, and one owner has exactly 4 in every draw. `adapter_slot_index`: A permutation: each slot holds exactly one adapter.
All inputs are finite; a program needn't handle non-finite values.
Results may differ from the reference program's by a relative error of at most 0.014.
Values may be sent and summed in bfloat16 or wider, within the bound.
A program may use at most 128 MiB of HBM per device.

```python
import jax
import jax.numpy as jnp

MODEL_WIDTH = 8192
QUERY_OUTPUTS = 8192
ADAPTER_RANK = 16
ADP_DEV = 32
BLOCK = 128
ADAPTER_COUNT = 512
FEAT = 1024
CAP = 4
BLOCKS = 32
TOKENS = 4096


def plan_draw(key):
    owner_count = ADAPTER_COUNT // ADP_DEV
    slot_table = jax.random.permutation(jax.random.fold_in(key, 101), jnp.arange(ADAPTER_COUNT, dtype=jnp.int32)).astype(jnp.int32)
    holder = jnp.argsort(slot_table, stable=True).astype(jnp.int32)
    hottest = jax.random.randint(jax.random.fold_in(key, 102), (), 0, owner_count, dtype=jnp.int32)
    seat_owner = jnp.arange((owner_count - 1) * CAP, dtype=jnp.int32) // CAP
    seat_owner = seat_owner + (seat_owner >= hottest).astype(jnp.int32)
    seat_owner = jax.random.permutation(jax.random.fold_in(key, 103), seat_owner)[:BLOCKS - CAP]
    owner_list = jnp.concatenate([jnp.full((CAP,), hottest, jnp.int32), seat_owner.astype(jnp.int32)])
    owner_list = jax.random.permutation(jax.random.fold_in(key, 104), owner_list)
    local_slot = jax.random.randint(jax.random.fold_in(key, 105), (BLOCKS,), 0, ADP_DEV, dtype=jnp.int32)
    adapters = holder[owner_list * ADP_DEV + local_slot]
    return (slot_table, adapters.astype(jnp.int32))


def draw_block_adapter_ids(key, part):
    return plan_draw(key)[1]


def draw_adapter_slot_index(key, part):
    return plan_draw(key)[0]


def touch_ends(drawn, stream_key, low, top_value):
    longest = drawn.shape.index(max(drawn.shape))
    spots = []
    for shift in (0, 1):
        where = [jax.random.randint(jax.random.fold_in(stream_key, axis), (), 0, length) for axis, length in enumerate(drawn.shape)]
        where[longest] = (where[longest] + shift) % drawn.shape[longest]
        spots.append(tuple(where))
    return drawn.at[spots[0]].set(low).at[spots[1]].set(top_value)


def levels(own_key, dims, cuts, low, largest):
    def one(position, blocks):
        draws = jax.random.uniform(jax.random.fold_in(jax.random.fold_in(own_key, 6), position), (blocks,), jnp.float32, low / len(cuts), largest / len(cuts))
        return jnp.repeat(jnp.exp(draws), dims[position] // blocks).reshape((-1,) + (1,) * (len(dims) - position - 1))

    factor_of = one(*cuts[0])
    for cut in cuts[1:]:
        factor_of = factor_of * one(*cut)
    return factor_of


def normal_values(rng, extent, spread, reach, pieces=(), held_as=jnp.bfloat16):
    array = spread * jax.random.normal(rng, extent, jnp.float32)
    if pieces:
        array = array * levels(rng, extent, pieces, -0.22, 0.18)
    return jnp.clip(array, -reach, reach).astype(held_as)


def setup_inputs(seed: int = 0, part: int = 0) -> dict:
    key_list = jax.random.split(jax.random.key(seed), 8)
    own_keys = jax.random.split(jax.random.fold_in(key_list[7], part), 8)
    tokens = normal_values(own_keys[0], (TOKENS, MODEL_WIDTH), 1.0, 6.0, ((0, 16), (1, 8)))
    query_weight = normal_values(key_list[1], (MODEL_WIDTH, QUERY_OUTPUTS), MODEL_WIDTH ** -0.5, 0.0625, ((0, 8), (1, 16)))
    adapter_down_weight = normal_values(key_list[2], (ADAPTER_COUNT, ADAPTER_RANK, MODEL_WIDTH), MODEL_WIDTH ** -0.5, 0.0625, ((0, 16), (2, 8)))
    adapter_up_weight = normal_values(key_list[3], (ADAPTER_COUNT, ADAPTER_RANK, QUERY_OUTPUTS), ADAPTER_RANK ** -0.5, 1.5, ((0, 16),))
    block_adapter_ids = draw_block_adapter_ids(jax.random.fold_in(jax.random.fold_in(key_list[7], part), 71), part)
    block_live_count = touch_ends(jax.random.randint(own_keys[5], (BLOCKS,), 1, BLOCK + 1), jax.random.fold_in(own_keys[5], 1), 1, BLOCK).astype(jnp.int32)
    adapter_slot_index = draw_adapter_slot_index(jax.random.fold_in(jax.random.fold_in(key_list[7], part), 71), part)
    return dict(tokens=tokens, query_weight=query_weight, adapter_down_weight=adapter_down_weight, adapter_up_weight=adapter_up_weight, block_adapter_ids=block_adapter_ids, block_live_count=block_live_count, adapter_slot_index=adapter_slot_index)


def reference(tokens, query_weight, adapter_down_weight, adapter_up_weight, block_adapter_ids, block_live_count, adapter_slot_index):
    block_slot_index = adapter_slot_index[block_adapter_ids].astype(jnp.int32)
    down_weight_blocks = adapter_down_weight[block_slot_index].astype(jnp.float32)
    up_weight_blocks = adapter_up_weight[block_slot_index].astype(jnp.float32)
    positions = jnp.arange(BLOCK, dtype=jnp.int32)
    live_mask = (positions[None, :] < block_live_count[:, None]).astype(jnp.float32)
    token_blocks = tokens.reshape(BLOCKS, BLOCK, MODEL_WIDTH).astype(jnp.float32)
    total = jnp.zeros((TOKENS, QUERY_OUTPUTS), jnp.float32)
    for slice_index in range(MODEL_WIDTH // FEAT):
        low_edge = slice_index * FEAT
        high_edge = low_edge + FEAT
        shrunk = jnp.einsum("ksd,krd->ksr", token_blocks[:, :, low_edge:high_edge], down_weight_blocks[:, :, low_edge:high_edge])
        shrunk = (shrunk * live_mask[:, :, None]).astype(jnp.bfloat16)
        adapter_part = jnp.einsum("ksr,krf->ksf", shrunk.astype(jnp.float32), up_weight_blocks).reshape(TOKENS, QUERY_OUTPUTS)
        base_part = jnp.dot(tokens[:, low_edge:high_edge], query_weight[low_edge:high_edge, :], preferred_element_type=jnp.float32)
        partial_value = (base_part + 2.0 * adapter_part).astype(jnp.bfloat16)
        total = total + partial_value.astype(jnp.float32)
    return total.astype(jnp.bfloat16)
```

```python
import functools

import jax
import jax.numpy as jnp
from jax import lax
from jax.experimental import pallas as pl
from jax.experimental.pallas import tpu as pltpu
from jax.sharding import PartitionSpec as P

MESH = pl.DeviceIdType.MESH
BLOCK = 128
CORES = 2
SUB = 8
LX = 1
LY = 1
SEATS = 4
adapter_scale = 2.0


def kernel(
    nx, ny,
    ids, live, slots, tok_h, w_h, dn_h, up_h,
    out,
    tok, w, dn, upv, prod, sb, rb, fin,
    u1s, u1r, u2s, u2r, shq, s1s, s1r, s2s, s2r,
    tab_slot, tab_seat,
    ld_sem, xs, xr, ds, dr, ys, yr,
    u1ss, u1rs, u2ss, u2rs, s1ss, s1rs, s2ss, s2rs,
):
    S = SUB
    R, Fe = tok.shape[3], tok.shape[4]
    half = Fe // 2
    N = w.shape[1]
    slots_dev = dn.shape[0]
    HX, HY = nx // 2, ny // 2
    NT = tok.shape[0]
    nblk = ids.shape[0]
    per_row = nblk // ny
    per_dev = per_row // CORES
    lanes = upv.shape[3]
    qpc = N // lanes

    ad = lax.axis_index("adapter")
    y = lax.axis_index("tensor")
    x = lax.div(ad, CORES)
    c = lax.rem(ad, CORES)
    oc = 1 - c

    def dev(dx=0, dy=0, core=None):
        core = c if core is None else core
        return {
            "adapter": lax.rem(x + (dx + nx) % nx, nx) * CORES + core,
            "tensor": lax.rem(y + (dy + ny) % ny, ny),
        }

    def rcopy(src, dst, ssem, rsem, where):
        return pltpu.make_async_remote_copy(
            src_ref=src, dst_ref=dst, send_sem=ssem, recv_sem=rsem,
            device_id=where, device_id_type=MESH,
        )

    def load_tok(s):
        return pltpu.make_async_copy(
            tok_h.at[pl.ds(s * R, R)], tok.at[s, 0, c], ld_sem.at[s]
        )

    def load_up(i):
        return pltpu.make_async_copy(
            up_h.at[:, :, pl.ds(pl.multiple_of(i * N * CORES + y * lanes, lanes), lanes)],
            upv.at[i], ld_sem.at[S + 2 + i],
        )

    load_w = pltpu.make_async_copy(w_h, w, ld_sem.at[S])
    load_dn = pltpu.make_async_copy(dn_h, dn, ld_sem.at[S + 1])
    for s in range(S):
        load_tok(s).start()
    load_w.start()
    load_dn.start()
    for i in range(nx):
        load_up(i).start()

    barrier = pltpu.get_barrier_semaphore()
    for where in (dev(1), dev(-1), dev(0, 1), dev(0, -1), dev(0, 0, oc)):
        pl.semaphore_signal(barrier, inc=1, device_id=where, device_id_type=MESH)
    pl.semaphore_wait(barrier, 5)

    def x_copy(way, d, s):
        off = (nx - d) % nx if way == 0 else d
        noff = nx - d - 1 if way == 0 else d + 1
        t = s + LX * d
        src = tok.at[t, off, c]
        dst = tok.at[t + LX, noff, c]
        if d == HX - 1:
            cols = pl.ds(way * half, half)
            src, dst = src.at[:, cols], dst.at[:, cols]
        return rcopy(
            src, dst, xs.at[way, d, s], xr.at[way, d, s], dev(1 if way == 0 else -1)
        )

    def core_copy(off, s):
        t = s + LX * min(off, nx - off)
        return rcopy(
            tok.at[t, off, c], tok.at[t, off, c], ds.at[off, s], dr.at[off, s],
            dev(0, 0, oc),
        )

    def core_wait(off, s):
        t = s + LX * min(off, nx - off)
        rcopy(
            tok.at[t, off, oc], tok.at[t, off, oc], ds.at[off, s], dr.at[off, s],
            dev(0, 0, oc),
        ).wait_recv()

    def own_send(s):
        load_tok(s).wait()
        x_copy(0, 0, s).start()
        x_copy(1, 0, s).start()
        core_copy(0, s).start()

    def y_copy(way, d, s):
        src, dst = sb.at[way, d - 1, s], rb.at[way, d - 1, s]
        if d == HY:
            src, dst = src.at[pl.ds(0, R)], dst.at[pl.ds(0, R)]
        return rcopy(
            src, dst, ys.at[way, d - 1, s], yr.at[way, d - 1, s],
            dev(0, 1 if way == 0 else -1),
        )

    own_send(0)

    def plan(k, seats):
        slot = slots[ids[k]]
        owner = lax.div(slot, slots_dev)
        tab_slot[k] = slot

        def count(i, n):
            return n + jnp.where(lax.div(tab_slot[i], slots_dev) == owner, 1, 0)

        seat = lax.fori_loop(0, k, count, jnp.int32(0))
        seat = jnp.minimum(seat, SEATS - 1)
        tab_seat[k] = seat
        mine = owner == ad
        return tuple(
            jnp.where(mine & (seat == q), k, seats[q]) for q in range(SEATS)
        )

    seat_blk = lax.fori_loop(0, nblk, plan, (jnp.int32(0),) * SEATS)

    load_w.wait()

    def u1_copy(i):
        return rcopy(u1s.at[i], u1r.at[i], u1ss.at[i], u1rs.at[i], dev(i))

    def up_first():
        for i in range(nx):
            load_up(i).wait()
        for q in range(SEATS):
            row = lax.rem(tab_slot[seat_blk[q]], slots_dev)
            for i in range(nx):
                v = upv[lax.rem(x + i, nx), row]
                if i == 0:
                    u1r[0, q] = v
                else:
                    u1s[i, q] = v
        for i in range(1, nx):
            u1_copy(i).start()

    dest_core = lax.div(y, qpc)
    y_in = lax.rem(y, qpc)

    def u2_copy(i):
        return rcopy(
            u2s.at[i], u2r.at[c, y_in], u2ss.at[i], u2rs.at[c, y_in],
            dev(0, i, dest_core),
        )

    def up_second():
        for i in range(1, nx):
            u1_copy(i).wait_recv()
        for i in range(ny):
            row = lax.rem(y + i, ny)
            for b in range(per_row):
                k = row * per_row + b
                owner = lax.div(tab_slot[k], slots_dev)
                rel = lax.rem(x - lax.div(owner, CORES) + nx, nx)
                v = u1r[rel, tab_seat[k]]
                keep = lax.rem(owner, CORES) == c
                u2s[i, b] = jnp.where(keep, v, jnp.zeros_like(v))
        for i in range(1, ny):
            u2_copy(i).start()

        @pl.when(dest_core == c)
        def _():
            u2r[c, y_in] = u2s[0]

        @pl.when(dest_core != c)
        def _():
            u2_copy(0).start()

    def s1_copy(hr, i):
        return rcopy(
            s1s.at[hr, i], s1r.at[hr, i], s1ss.at[hr, i], s1rs.at[hr, i],
            dev(0, i, c if hr == 0 else oc),
        )

    def shrink_first():
        load_dn.wait()
        for q in range(SEATS):
            k = seat_blk[q]
            a = lax.div(k, per_dev)
            piece = lax.rem(k, per_dev)
            off = lax.rem(lax.div(a, CORES) - x + nx, nx)
            dist = jnp.minimum(off, nx - off)
            ca = lax.rem(a, CORES)
            n_sub = S // per_dev
            rows = [
                tok[piece * n_sub + i + LX * dist, off, ca] for i in range(n_sub)
            ]
            rows = jnp.concatenate(rows, axis=0) if n_sub > 1 else rows[0]
            weight = dn[lax.rem(tab_slot[k], slots_dev)]
            v = lax.dot_general(
                weight, rows, (((1,), (1,)), ((), ())),
                preferred_element_type=jnp.float32,
            )
            pos = lax.broadcasted_iota(jnp.int32, v.shape, 1)
            shq[q] = jnp.where(pos < live[k], v, 0.0).astype(shq.dtype)
        for i in range(ny):
            row = lax.rem(y + i, ny)
            for hr in range(CORES):
                h = c if hr == 0 else oc
                for b in range(per_dev):
                    k = row * per_row + h * per_dev + b
                    v = shq[tab_seat[k]]
                    v = jnp.where(
                        lax.div(tab_slot[k], slots_dev) == ad, v, jnp.zeros_like(v)
                    )
                    if hr == 0 and i == 0:
                        s1r[0, 0, b] = v
                    else:
                        s1s[hr, i, b] = v
        for i in range(ny):
            for hr in range(CORES):
                if hr or i:
                    s1_copy(hr, i).start()

    def s2_copy(hr, i):
        return rcopy(
            s2s, s2r.at[hr, i], s2ss.at[hr, i], s2rs.at[hr, i],
            dev(i, 0, c if hr == 0 else oc),
        )

    def shrink_second():
        for i in range(ny):
            for hr in range(CORES):
                if hr or i:
                    s1_copy(hr, i).wait_recv()
        v = jnp.sum(s1r[...].astype(jnp.float32), axis=(0, 1)).astype(s2s.dtype)
        s2s[...] = v
        s2r[0, 0] = v
        for i in range(nx):
            for hr in range(CORES):
                if hr or i:
                    s2_copy(hr, i).start()

    y_order = [HY]
    for d in range(HY - 1, 0, -1):
        y_order += [d, ny - d]
    y_order += [0]

    def tick(t, carry):
        for d in range(HX, 0, -1):
            s = t - LX * d

            @pl.when((s >= 0) & (s < S))
            def _(d=d, s=s):
                for way in range(2):
                    x_copy(way, d - 1, s).wait_recv()
                    if d < HX:
                        x_copy(way, d, s).start()
                if d < HX:
                    core_copy(nx - d, s).start()
                core_copy(d, s).start()

        @pl.when(t + 1 < S)
        def _():
            own_send(t + 1)

        for d in range(HX + 1):
            s = t - LX * d

            @pl.when((s >= 0) & (s < S))
            def _(d=d, s=s):
                core_wait(d, s)
                if 0 < d < HX:
                    core_wait(nx - d, s)

        @pl.when(t < NT)
        def _():
            v = jnp.dot(
                tok[t].reshape(nx * CORES * R, Fe), w[...],
                preferred_element_type=jnp.float32,
            )
            prod[t] = v.reshape(nx, CORES * R, N)

        for o in y_order:
            d = min(o, ny - o)
            way = 0 if o <= HY else 1
            off = lax.rem(lax.rem(y + o, ny) - x + nx, nx)
            dx = jnp.minimum(off, nx - off)
            s = t - LX * dx - LY * (HY - d)

            @pl.when((s >= 0) & (s < S))
            def _(o=o, d=d, way=way, off=off, dx=dx, s=s):
                v = prod.at[s + LX * dx, off]
                top, low = pl.ds(0, R), pl.ds(R, R)
                dt = sb.dtype
                if d == HY:
                    sb[0, d - 1, s, top] = v[top].astype(dt)
                    sb[1, d - 1, s, top] = v[low].astype(dt)
                    y_copy(0, d, s).start()
                    y_copy(1, d, s).start()
                elif d == HY - 1:
                    y_copy(way, d + 1, s).wait_recv()
                    got = rb[way, d, s, top].astype(jnp.float32)
                    add, keep = (top, low) if way == 0 else (low, top)
                    sb[way, d - 1, s, add] = (v[add] + got).astype(dt)
                    sb[way, d - 1, s, keep] = v[keep].astype(dt)
                    y_copy(way, d, s).start()
                elif d > 0:
                    y_copy(way, d + 1, s).wait_recv()
                    got = rb[way, d, s].astype(jnp.float32)
                    sb[way, d - 1, s] = (v[...] + got).astype(dt)
                    y_copy(way, d, s).start()
                else:
                    y_copy(0, 1, s).wait_recv()
                    y_copy(1, 1, s).wait_recv()
                    total = (
                        v[...]
                        + rb[0, 0, s].astype(jnp.float32)
                        + rb[1, 0, s].astype(jnp.float32)
                    )
                    fin[0, s] = total[:R]
                    fin[1, s] = total[R:]

        @pl.when(t == LX * HX + 1)
        def _():
            up_first()

        @pl.when(t == NT - 2)
        def _():
            up_second()

        @pl.when(t == NT - 1)
        def _():
            shrink_first()

        @pl.when(t == NT + 1)
        def _():
            shrink_second()

        return carry

    lax.fori_loop(0, NT + LY * HY, tick, 0)

    for p in range(qpc):
        for cs in range(CORES):
            own = (c == cs) & (y == c * qpc + p)

            @pl.when(jnp.logical_not(own))
            def _(cs=cs, p=p):
                rcopy(
                    u2s.at[0], u2r.at[cs, p], u2ss.at[0], u2rs.at[cs, p], dev(0, 0, oc)
                ).wait_recv()

    for i in range(nx):
        for hr in range(CORES):
            if hr or i:
                s2_copy(hr, i).wait_recv()
    ups = u2r[0] + u2r[1]
    for hr in range(CORES):
        h = c if hr == 0 else oc
        sh = s2r[hr, 0]
        for i in range(1, nx):
            sh = sh + s2r[hr, i]
        n_sub = S // per_dev
        for b in range(per_dev):
            blk = h * per_dev + b
            up = jnp.concatenate(
                [u2r[0, p, blk] + u2r[1, p, blk] for p in range(qpc)], axis=1
            )
            part = lax.dot_general(
                sh[b], up, (((0,), (0,)), ((), ())),
                preferred_element_type=jnp.float32,
            )
            base = fin[h, pl.ds(b * n_sub, n_sub)].reshape(n_sub * R, N)
            start = pl.multiple_of(h * (S * R) + b * BLOCK, BLOCK)
            out[pl.ds(start, BLOCK), :] = (base + adapter_scale * part).astype(out.dtype)

    def drain(s, carry):
        for d in range(HX):
            x_copy(0, d, s).wait_send()
            x_copy(1, d, s).wait_send()
        for off in range(nx):
            core_copy(off, s).wait_send()
        for d in range(1, HY + 1):
            y_copy(0, d, s).wait_send()
            y_copy(1, d, s).wait_send()
        return carry

    lax.fori_loop(0, S, drain, 0)
    for i in range(1, nx):
        u1_copy(i).wait_send()
    for i in range(1, ny):
        u2_copy(i).wait_send()

    @pl.when(dest_core != c)
    def _():
        u2_copy(0).wait_send()

    for i in range(ny):
        for hr in range(CORES):
            if hr or i:
                s1_copy(hr, i).wait_send()
    for i in range(nx):
        for hr in range(CORES):
            if hr or i:
                s2_copy(hr, i).wait_send()


def on_device(tokens, query_weight, down, up, ids, live, slots):
    nx = lax.axis_size("adapter") // CORES
    ny = lax.axis_size("tensor")
    rows, Fe = tokens.shape
    N = query_weight.shape[1]
    slots_dev, rank = down.shape[0], down.shape[1]
    R = rows // SUB
    NT = SUB + LX * (nx // 2)
    HX, HY = nx // 2, ny // 2
    lanes = N * CORES // ny
    qpc = N // lanes
    per_row = ids.shape[0] // ny
    per_dev = per_row // CORES
    bf = jnp.bfloat16
    dma = pltpu.SemaphoreType.DMA
    smem = pl.BlockSpec(memory_space=pltpu.SMEM)
    hbm = pl.BlockSpec(memory_space=pl.ANY)
    piece = (per_dev, rank, BLOCK)
    return pl.pallas_call(
        functools.partial(kernel, nx, ny),
        out_shape=jax.ShapeDtypeStruct((CORES * rows, N), bf),
        in_specs=[smem] * 3 + [hbm] * 4,
        out_specs=pl.BlockSpec(memory_space=pltpu.VMEM),
        scratch_shapes=[
            pltpu.VMEM((NT, nx, CORES, R, Fe), bf),
            pltpu.VMEM((Fe, N), bf),
            pltpu.VMEM((slots_dev, rank, Fe), bf),
            pltpu.VMEM((nx, slots_dev, rank, lanes), bf),
            pltpu.VMEM((NT, nx, CORES * R, N), jnp.float32),
            pltpu.VMEM((2, HY, SUB, CORES * R, N), bf),
            pltpu.VMEM((2, HY, SUB, CORES * R, N), bf),
            pltpu.VMEM((CORES, SUB, R, N), jnp.float32),
            pltpu.VMEM((nx, SEATS, rank, lanes), bf),
            pltpu.VMEM((nx, SEATS, rank, lanes), bf),
            pltpu.VMEM((ny, per_row, rank, lanes), bf),
            pltpu.VMEM((CORES, qpc, per_row, rank, lanes), bf),
            pltpu.VMEM((SEATS, rank, BLOCK), bf),
            pltpu.VMEM((CORES, ny) + piece, bf),
            pltpu.VMEM((CORES, ny) + piece, bf),
            pltpu.VMEM(piece, bf),
            pltpu.VMEM((CORES, nx) + piece, bf),
            pltpu.SMEM((ids.shape[0],), jnp.int32),
            pltpu.SMEM((ids.shape[0],), jnp.int32),
            dma((SUB + 2 + nx,)),
            dma((2, HX, SUB)), dma((2, HX, SUB)),
            dma((nx, SUB)), dma((nx, SUB)),
            dma((2, HY, SUB)), dma((2, HY, SUB)),
            dma((nx,)), dma((nx,)),
            dma((ny,)), dma((CORES, qpc)),
            dma((CORES, ny)), dma((CORES, ny)),
            dma((CORES, nx)), dma((CORES, nx)),
        ],
        compiler_params=pltpu.CompilerParams(
            collective_id=0, has_side_effects=True,
            vmem_limit_bytes=60 * 1024 * 1024,
        ),
    )(ids, live, slots, tokens, query_weight, down, up)


def solution(mesh):
    placed = (
        P(("groups", "adapter"), "tensor"),
        P("tensor", "adapter"),
        P("adapter", None, "tensor"),
        P("adapter", None, None),
        P("groups"),
        P("groups"),
        P("groups"),
    )
    return jax.shard_map(
        on_device,
        mesh=mesh,
        in_specs=placed,
        out_specs=P(("groups", "tensor"), "adapter"),
        check_vma=False,
    )
```

```python
import functools

import jax
import jax.numpy as jnp
from jax import lax
from jax.experimental import pallas as pl
from jax.experimental.pallas import tpu as pltpu
from jax.sharding import PartitionSpec as P

MESH = pl.DeviceIdType.MESH
BLOCK = 128
CORES = 2
SUB = 16
LX = 2
LY = 2
LAG = 2
AHEAD = 1
SEATS = 4
UP1 = 8
UP2 = 20
SH2 = 3
adapter_scale = 2.0


def kernel(
    nx, ny,
    ids, live, slots, tok_h, w_h, dn_h, up_h,
    out,
    tok, w, dn, upv, prod, sb, rb, fin,
    u1s, u1r, u2s, u2r, shq, s1s, s1r, s2s, s2r,
    tab_owner, tab_row, tab_seat,
    obuf, st_sem, ld_sem, xs, xr, ds, dr, ys, yr,
    u1ss, u1rs, u2ss, u2rs, s1ss, s1rs, s2ss, s2rs,
):
    S = SUB
    R, Fe = tok.shape[3], tok.shape[4]
    half = Fe // 2
    N = w.shape[1]
    slots_dev = dn.shape[0]
    HX, HY = nx // 2, ny // 2
    NT = tok.shape[0]
    nblk = ids.shape[0]
    per_row = nblk // ny
    per_dev = per_row // CORES
    lanes = upv.shape[3]
    qpc = N // lanes

    ad = lax.axis_index("adapter")
    y = lax.axis_index("tensor")
    x = lax.div(ad, CORES)
    c = lax.rem(ad, CORES)
    oc = 1 - c

    def dev(dx=0, dy=0, core=None):
        core = c if core is None else core
        return {
            "adapter": lax.rem(x + (dx + nx) % nx, nx) * CORES + core,
            "tensor": lax.rem(y + (dy + ny) % ny, ny),
        }

    def rcopy(src, dst, ssem, rsem, where):
        return pltpu.make_async_remote_copy(
            src_ref=src, dst_ref=dst, send_sem=ssem, recv_sem=rsem,
            device_id=where, device_id_type=MESH,
        )

    load_tok = pltpu.make_async_copy(tok_h, tok.at[pl.ds(0, S), 0, c], ld_sem.at[0])

    def load_up(i):
        return pltpu.make_async_copy(
            up_h.at[:, :, pl.ds(pl.multiple_of(i * N * CORES + y * lanes, lanes), lanes)],
            upv.at[i], ld_sem.at[3],
        )

    load_w = pltpu.make_async_copy(w_h, w, ld_sem.at[1])
    load_dn = pltpu.make_async_copy(dn_h, dn, ld_sem.at[2])
    load_tok.start()
    load_w.start()
    load_dn.start()
    for i in range(nx):
        load_up(i).start()

    barrier = pltpu.get_barrier_semaphore()
    for where in (dev(1), dev(-1), dev(0, 1), dev(0, -1), dev(0, 0, oc)):
        pl.semaphore_signal(barrier, inc=1, device_id=where, device_id_type=MESH)
    pl.semaphore_wait(barrier, 5)

    def x_copy(way, d, s):
        off = (nx - d) % nx if way == 0 else d
        noff = nx - d - 1 if way == 0 else d + 1
        t = s + LX * d
        src = tok.at[t, off, c]
        dst = tok.at[t + LX, noff, c]
        if d == HX - 1:
            cols = pl.ds(way * half, half)
            src, dst = src.at[:, cols], dst.at[:, cols]
        return rcopy(
            src, dst, xs.at[way, 1 if d == HX - 1 else 0], xr.at[way, d, s],
            dev(1 if way == 0 else -1),
        )

    def core_copy(t, core):
        part = tok.at[t, :, core]
        return rcopy(part, part, ds.at[0], dr.at[t], dev(0, 0, oc))

    def own_send(s):
        x_copy(0, 0, s).start()
        x_copy(1, 0, s).start()

    def y_copy(way, d, s):
        src, dst = sb.at[way, d - 1, s], rb.at[way, d - 1, s]
        if d == HY:
            src, dst = src.at[pl.ds(0, R)], dst.at[pl.ds(0, R)]
        return rcopy(
            src, dst, ys.at[way, 1 if d == HY else 0], yr.at[way, d - 1, s],
            dev(0, 1 if way == 0 else -1),
        )

    load_tok.wait()
    for s in range(AHEAD):
        own_send(s)

    def place(k, carry):
        slot = slots[ids[k]]
        tab_owner[k] = lax.div(slot, slots_dev)
        tab_row[k] = lax.rem(slot, slots_dev)
        return carry

    lax.fori_loop(0, nblk, place, 0)

    def plan(k, seats):
        owner = tab_owner[k]
        seat = jnp.int32(0)
        for i in range(nblk):
            seat += jnp.where((tab_owner[i] == owner) & (i < k), 1, 0)
        seat = jnp.minimum(seat, SEATS - 1)
        tab_seat[k] = seat
        mine = owner == ad
        return tuple(
            jnp.where(mine & (seat == q), k, seats[q]) for q in range(SEATS)
        )

    seat_blk = lax.fori_loop(0, nblk, plan, (jnp.int32(0),) * SEATS)

    load_w.wait()

    def u1_copy(i):
        return rcopy(u1s.at[i], u1r.at[i], u1ss.at[0], u1rs.at[0], dev(i))

    def up_first():
        pltpu.make_async_copy(upv, upv, ld_sem.at[3]).wait()
        for q in range(SEATS):
            row = tab_row[seat_blk[q]]
            for i in range(nx):
                v = upv[lax.rem(x + i, nx), row]
                if i == 0:
                    u1r[0, q] = v
                else:
                    u1s[i, q] = v
        for i in range(1, nx):
            u1_copy(i).start()

    dest_core = lax.div(y, qpc)
    y_in = lax.rem(y, qpc)

    def u2_copy(i):
        return rcopy(
            u2s.at[i], u2r.at[c, y_in], u2ss.at[min(i, 1)], u2rs.at[c, y_in],
            dev(0, i, dest_core),
        )

    def up_second():
        rest = u1r.at[pl.ds(1, nx - 1)]
        rcopy(rest, rest, u1ss.at[0], u1rs.at[0], dev(1)).wait_recv()
        for i in range(ny):
            row = lax.rem(y + i, ny)
            for b in range(per_row):
                k = row * per_row + b
                owner = tab_owner[k]
                rel = lax.rem(x - lax.div(owner, CORES) + nx, nx)
                v = u1r[rel, tab_seat[k]]
                keep = lax.rem(owner, CORES) == c
                u2s[i, b] = jnp.where(keep, v, jnp.zeros_like(v))
        for i in range(1, ny):
            u2_copy(i).start()

        @pl.when(dest_core == c)
        def _():
            u2r[c, y_in] = u2s[0]

        @pl.when(dest_core != c)
        def _():
            u2_copy(0).start()

    def s1_copy(hr, i):
        return rcopy(
            s1s.at[hr, i], s1r.at[hr, i], s1ss.at[hr], s1rs.at[hr],
            dev(0, i, c if hr == 0 else oc),
        )

    def shrink_first():
        load_dn.wait()
        for q in range(SEATS):
            k = seat_blk[q]
            a = lax.div(k, per_dev)
            piece = lax.rem(k, per_dev)
            off = lax.rem(lax.div(a, CORES) - x + nx, nx)
            dist = jnp.minimum(off, nx - off)
            ca = lax.rem(a, CORES)
            n_sub = S // per_dev
            rows = [
                tok[piece * n_sub + i + LX * dist, off, ca] for i in range(n_sub)
            ]
            rows = jnp.concatenate(rows, axis=0) if n_sub > 1 else rows[0]
            weight = dn[tab_row[k]]
            v = lax.dot_general(
                weight, rows, (((1,), (1,)), ((), ())),
                preferred_element_type=jnp.float32,
            )
            pos = lax.broadcasted_iota(jnp.int32, v.shape, 1)
            shq[q] = jnp.where(pos < live[k], v, 0.0).astype(shq.dtype)
        for i in range(ny):
            row = lax.rem(y + i, ny)
            for hr in range(CORES):
                h = c if hr == 0 else oc
                for b in range(per_dev):
                    k = row * per_row + h * per_dev + b
                    v = shq[tab_seat[k]]
                    v = jnp.where(tab_owner[k] == ad, v, jnp.zeros_like(v))
                    if hr == 0 and i == 0:
                        s1r[0, 0, b] = v
                    else:
                        s1s[hr, i, b] = v
        for i in range(ny):
            for hr in range(CORES):
                if hr or i:
                    s1_copy(hr, i).start()

    def s2_copy(hr, i):
        return rcopy(
            s2s, s2r.at[hr, i], s2ss.at[hr], s2rs.at[hr],
            dev(i, 0, c if hr == 0 else oc),
        )

    def shrink_second():
        for hr in range(CORES):
            got = s1r.at[hr, pl.ds(1 - hr, ny - 1 + hr)]
            rcopy(got, got, s1ss.at[hr], s1rs.at[hr], dev(0, 0, oc)).wait_recv()
        v = jnp.sum(s1r[...].astype(jnp.float32), axis=(0, 1)).astype(s2s.dtype)
        s2s[...] = v
        s2r[0, 0] = v
        for i in range(nx):
            for hr in range(CORES):
                if hr or i:
                    s2_copy(hr, i).start()

    def chain(o, t):
        d = min(o, ny - o)
        way = 0 if o <= HY else 1
        off = lax.rem(lax.rem(y + o, ny) - x + nx, nx)
        dx = jnp.minimum(off, nx - off)
        s = t - LX * dx - LY * (HY - d) - LAG

        @pl.when((s >= 0) & (s < S))
        def _():
            v = prod.at[s + LX * dx, off]
            top, low = pl.ds(0, R), pl.ds(R, R)
            dt = sb.dtype
            if d == HY:
                sb[0, d - 1, s, top] = v[top].astype(dt)
                sb[1, d - 1, s, top] = v[low].astype(dt)
                y_copy(0, d, s).start()
                y_copy(1, d, s).start()
            elif d == HY - 1:
                add, keep = (top, low) if way == 0 else (low, top)
                sb[way, d - 1, s, keep] = v[keep].astype(dt)
                y_copy(way, d + 1, s).wait_recv()
                got = rb[way, d, s, top].astype(jnp.float32)
                sb[way, d - 1, s, add] = (v[add] + got).astype(dt)
                y_copy(way, d, s).start()
            elif d > 0:
                y_copy(way, d + 1, s).wait_recv()
                got = rb[way, d, s].astype(jnp.float32)
                sb[way, d - 1, s] = (v[...] + got).astype(dt)
                y_copy(way, d, s).start()
            else:
                y_copy(0, 1, s).wait_recv()
                y_copy(1, 1, s).wait_recv()
                total = (
                    v[...]
                    + rb[0, 0, s].astype(jnp.float32)
                    + rb[1, 0, s].astype(jnp.float32)
                )
                fin[0, s] = total[:R]
                fin[1, s] = total[R:]

    def forward(d, t):
        s = t - LX * d

        @pl.when((s >= 0) & (s < S))
        def _():
            for way in range(2):
                x_copy(way, d - 1, s).wait_recv()
                if d < HX:
                    x_copy(way, d, s).start()

    def tick(t, carry):
        @pl.when(t == NT + SH2)
        def _():
            shrink_second()

        for k in range(max(HX, HY)):
            if k < HX:
                forward(HX - k, t)
            if k < HY:
                for o in sorted({HY - k, ny - HY + k}):
                    chain(o, t)

        @pl.when(t + AHEAD < S)
        def _():
            own_send(t + AHEAD)

        chain(0, t)

        @pl.when(t < NT)
        def _():
            core_copy(t, c).start()

        @pl.when((t >= 1) & (t <= NT))
        def _():
            core_copy(t - 1, oc).wait_recv()
            v = jnp.dot(
                tok[t - 1].reshape(nx * CORES * R, Fe), w[...],
                preferred_element_type=jnp.float32,
            )
            prod[t - 1] = v.reshape(nx, CORES * R, N)

        @pl.when(t == UP1)
        def _():
            up_first()

        @pl.when(t == UP2)
        def _():
            up_second()

        @pl.when(t == NT)
        def _():
            shrink_first()

        return carry

    lax.fori_loop(0, NT + LY * HY + LAG, tick, 0)

    for p in range(qpc):
        for cs in range(CORES):
            own = (c == cs) & (y == c * qpc + p)

            @pl.when(jnp.logical_not(own))
            def _(cs=cs, p=p):
                rcopy(
                    u2s.at[0], u2r.at[cs, p], u2ss.at[0], u2rs.at[cs, p], dev(0, 0, oc)
                ).wait_recv()

    for hr in range(CORES):
        got = s2r.at[hr, pl.ds(1 - hr, nx - 1 + hr)]
        rcopy(got, got, s2ss.at[hr], s2rs.at[hr], dev(0, 0, oc)).wait_recv()
    stores = []
    for hr in range(CORES):
        h = c if hr == 0 else oc
        sh = s2r[hr, 0]
        for i in range(1, nx):
            sh = sh + s2r[hr, i]
        n_sub = S // per_dev
        for b in range(per_dev):
            blk = h * per_dev + b
            up = jnp.concatenate(
                [u2r[0, p, blk] + u2r[1, p, blk] for p in range(qpc)], axis=1
            )
            part = lax.dot_general(
                sh[b], up, (((0,), (0,)), ((), ())),
                preferred_element_type=jnp.float32,
            )
            base = fin[h, pl.ds(b * n_sub, n_sub)].reshape(n_sub * R, N)
            start = pl.multiple_of(h * (S * R) + b * BLOCK, BLOCK)
            obuf[hr, b] = (base + adapter_scale * part).astype(out.dtype)
            store = pltpu.make_async_copy(
                obuf.at[hr, b], out.at[pl.ds(start, BLOCK)], st_sem.at[hr, b]
            )
            store.start()
            stores.append(store)

    for store in stores:
        store.wait()

    def sent(ref, sem):
        rcopy(ref, ref, sem, dr.at[0], dev(0, 0, oc)).wait_send()

    for way in range(2):
        sent(tok.at[pl.ds(0, S), pl.ds(0, HX - 1), c], xs.at[way, 0])
        sent(tok.at[pl.ds(0, S), 0, c, :, pl.ds(0, half)], xs.at[way, 1])
        sent(sb.at[way, pl.ds(0, HY - 1)], ys.at[way, 0])
        sent(sb.at[way, HY - 1, :, pl.ds(0, R)], ys.at[way, 1])
    sent(tok.at[:, :, c], ds.at[0])
    sent(u1s.at[pl.ds(1, nx - 1)], u1ss.at[0])
    sent(u2s.at[pl.ds(1, ny - 1)], u2ss.at[1])

    @pl.when(dest_core != c)
    def _():
        u2_copy(0).wait_send()

    for hr in range(CORES):
        sent(s1s.at[hr, pl.ds(1 - hr, ny - 1 + hr)], s1ss.at[hr])
        sent(s2r.at[hr, pl.ds(1 - hr, nx - 1 + hr)], s2ss.at[hr])


def on_device(tokens, query_weight, down, up, ids, live, slots):
    nx = lax.axis_size("adapter") // CORES
    ny = lax.axis_size("tensor")
    rows, Fe = tokens.shape
    N = query_weight.shape[1]
    slots_dev, rank = down.shape[0], down.shape[1]
    R = rows // SUB
    NT = SUB + LX * (nx // 2)
    HX, HY = nx // 2, ny // 2
    lanes = N * CORES // ny
    qpc = N // lanes
    per_row = ids.shape[0] // ny
    per_dev = per_row // CORES
    bf = jnp.bfloat16
    dma = pltpu.SemaphoreType.DMA
    smem = pl.BlockSpec(memory_space=pltpu.SMEM)
    hbm = pl.BlockSpec(memory_space=pl.ANY)
    piece = (per_dev, rank, BLOCK)
    return pl.pallas_call(
        functools.partial(kernel, nx, ny),
        out_shape=jax.ShapeDtypeStruct((CORES * rows, N), bf),
        in_specs=[smem] * 3 + [hbm] * 4,
        out_specs=hbm,
        scratch_shapes=[
            pltpu.VMEM((NT, nx, CORES, R, Fe), bf),
            pltpu.VMEM((Fe, N), bf),
            pltpu.VMEM((slots_dev, rank, Fe), bf),
            pltpu.VMEM((nx, slots_dev, rank, lanes), bf),
            pltpu.VMEM((NT, nx, CORES * R, N), jnp.float32),
            pltpu.VMEM((2, HY, SUB, CORES * R, N), bf),
            pltpu.VMEM((2, HY, SUB, CORES * R, N), bf),
            pltpu.VMEM((CORES, SUB, R, N), jnp.float32),
            pltpu.VMEM((nx, SEATS, rank, lanes), bf),
            pltpu.VMEM((nx, SEATS, rank, lanes), bf),
            pltpu.VMEM((ny, per_row, rank, lanes), bf),
            pltpu.VMEM((CORES, qpc, per_row, rank, lanes), bf),
            pltpu.VMEM((SEATS, rank, BLOCK), bf),
            pltpu.VMEM((CORES, ny) + piece, bf),
            pltpu.VMEM((CORES, ny) + piece, bf),
            pltpu.VMEM(piece, bf),
            pltpu.VMEM((CORES, nx) + piece, bf),
            pltpu.SMEM((ids.shape[0],), jnp.int32),
            pltpu.SMEM((ids.shape[0],), jnp.int32),
            pltpu.SMEM((ids.shape[0],), jnp.int32),
            pltpu.VMEM((CORES, per_dev, BLOCK, N), bf),
            dma((CORES, per_dev)),
            dma((4,)),
            dma((2, 2)), dma((2, HX, SUB)),
            dma((1,)), dma((NT,)),
            dma((2, 2)), dma((2, HY, SUB)),
            dma((1,)), dma((1,)),
            dma((2,)), dma((CORES, qpc)),
            dma((CORES,)), dma((CORES,)),
            dma((CORES,)), dma((CORES,)),
        ],
        compiler_params=pltpu.CompilerParams(
            collective_id=0, has_side_effects=True,
            vmem_limit_bytes=60 * 1024 * 1024,
        ),
    )(ids, live, slots, tokens.reshape(SUB, R, Fe), query_weight, down, up)


def solution(mesh):
    placed = (
        P(("groups", "adapter"), "tensor"),
        P("tensor", "adapter"),
        P("adapter", None, "tensor"),
        P("adapter", None, None),
        P("groups"),
        P("groups"),
        P("groups"),
    )
    return jax.shard_map(
        on_device,
        mesh=mesh,
        in_specs=placed,
        out_specs=P(("groups", "tensor"), "adapter"),
        check_vma=False,
    )
```

```python
import functools

import jax
import jax.numpy as jnp
from jax import lax
from jax.experimental import pallas as pl
from jax.experimental.pallas import tpu as pltpu
from jax.sharding import PartitionSpec as P

MESH = pl.DeviceIdType.MESH
BLOCK = 128
CORES = 2
SUB = 16
LX = 2
LY = 2
LAG = 2
AHEAD = 1
SEATS = 4
UP1 = 1
UP2 = 6
SH2 = 3
adapter_scale = 2.0


def kernel(
    nx, ny,
    ids, live, slots, tok_h, w_h, dn_h, up_h,
    out,
    tok, w, dn, upv, prod, sb, rb, fin,
    u1s, u1r, u2s, u2r, shq, s1s, s1r, s2s, s2r,
    tab_owner, tab_row, tab_seat,
    obuf, st_sem, ld_sem, xs, xr, ds, dr, ys, yr,
    u1ss, u1rs, u2ss, u2rs, s1ss, s1rs, s2ss, s2rs,
):
    S = SUB
    R, Fe = tok.shape[3], tok.shape[4]
    half = Fe // 2
    N = w.shape[1]
    slots_dev = dn.shape[0]
    HX, HY = nx // 2, ny // 2
    NT = tok.shape[0]
    nblk = ids.shape[0]
    per_row = nblk // ny
    per_dev = per_row // CORES
    lanes = upv.shape[3]
    qpc = N // lanes

    ad = lax.axis_index("adapter")
    y = lax.axis_index("tensor")
    x = lax.div(ad, CORES)
    c = lax.rem(ad, CORES)
    oc = 1 - c

    def dev(dx=0, dy=0, core=None):
        core = c if core is None else core
        return {
            "adapter": lax.rem(x + (dx + nx) % nx, nx) * CORES + core,
            "tensor": lax.rem(y + (dy + ny) % ny, ny),
        }

    def rcopy(src, dst, ssem, rsem, where):
        return pltpu.make_async_remote_copy(
            src_ref=src, dst_ref=dst, send_sem=ssem, recv_sem=rsem,
            device_id=where, device_id_type=MESH,
        )

    load_tok = pltpu.make_async_copy(tok_h, tok.at[pl.ds(0, S), 0, c], ld_sem.at[0])

    def load_up(i):
        return pltpu.make_async_copy(
            up_h.at[:, :, pl.ds(pl.multiple_of(i * N * CORES + y * lanes, lanes), lanes)],
            upv.at[i], ld_sem.at[3],
        )

    load_w = pltpu.make_async_copy(w_h, w, ld_sem.at[1])
    load_dn = pltpu.make_async_copy(dn_h, dn, ld_sem.at[2])
    load_tok.start()
    load_w.start()
    load_dn.start()
    for i in range(nx):
        load_up(i).start()

    barrier = pltpu.get_barrier_semaphore()
    peers = [(i, 0) for i in range(nx)] + [(0, i) for i in range(1, ny)]
    for px, py in peers:
        for core in (c, oc):
            if px or py or core is oc:
                pl.semaphore_signal(
                    barrier, inc=1, device_id=dev(px, py, core), device_id_type=MESH
                )
    pl.semaphore_wait(barrier, CORES * len(peers) - 1)

    def x_copy(way, d, s):
        off = (nx - d) % nx if way == 0 else d
        noff = nx - d - 1 if way == 0 else d + 1
        t = s + LX * d
        src = tok.at[t, off, c]
        dst = tok.at[t + LX, noff, c]
        if d == HX - 1:
            cols = pl.ds(way * half, half)
            src, dst = src.at[:, cols], dst.at[:, cols]
        return rcopy(
            src, dst, xs.at[way, 1 if d == HX - 1 else 0], xr.at[d, s],
            dev(1 if way == 0 else -1),
        )

    def core_copy(t, core):
        part = tok.at[t, :, core]
        return rcopy(part, part, ds.at[0], dr.at[t], dev(0, 0, oc))

    def own_send(s):
        x_copy(0, 0, s).start()
        x_copy(1, 0, s).start()

    def y_copy(way, d, s):
        src, dst = sb.at[way, d - 1, s], rb.at[way, d - 1, s]
        if d == HY:
            src, dst = src.at[pl.ds(0, R)], dst.at[pl.ds(0, R)]
        return rcopy(
            src, dst, ys.at[way, 1 if d == HY else 0],
            yr.at[0 if d == 1 else d - 1 + way * (HY - 1), s],
            dev(0, 1 if way == 0 else -1),
        )

    load_tok.wait()
    for s in range(AHEAD):
        own_send(s)

    def place(k, carry):
        slot = slots[ids[k]]
        tab_owner[k] = lax.div(slot, slots_dev)
        tab_row[k] = lax.rem(slot, slots_dev)
        return carry

    lax.fori_loop(0, nblk, place, 0)

    def plan(k, seats):
        owner = tab_owner[k]
        seat = jnp.int32(0)
        for i in range(nblk):
            seat += jnp.where((tab_owner[i] == owner) & (i < k), 1, 0)
        seat = jnp.minimum(seat, SEATS - 1)
        tab_seat[k] = seat
        mine = owner == ad
        return tuple(
            jnp.where(mine & (seat == q), k, seats[q]) for q in range(SEATS)
        )

    seat_blk = lax.fori_loop(0, nblk, plan, (jnp.int32(0),) * SEATS)

    load_w.wait()

    def u1_copy(i):
        return rcopy(u1s.at[i], u1r.at[i], u1ss.at[0], u1rs.at[0], dev(i))

    def up_first():
        pltpu.make_async_copy(upv, upv, ld_sem.at[3]).wait()
        for q in range(SEATS):
            row = tab_row[seat_blk[q]]
            for i in range(nx):
                v = upv[lax.rem(x + i, nx), row]
                if i == 0:
                    u1r[0, q] = v
                else:
                    u1s[i, q] = v
        for i in range(1, nx):
            u1_copy(i).start()

    dest_core = lax.div(y, qpc)
    y_in = lax.rem(y, qpc)

    def u2_copy(i):
        return rcopy(
            u2s.at[i], u2r.at[c, y_in], u2ss.at[min(i, 1)], u2rs.at[c, y_in],
            dev(0, i, dest_core),
        )

    def up_second():
        rest = u1r.at[pl.ds(1, nx - 1)]
        rcopy(rest, rest, u1ss.at[0], u1rs.at[0], dev(1)).wait_recv()
        for i in range(ny):
            row = lax.rem(y + i, ny)
            for b in range(per_row):
                k = row * per_row + b
                owner = tab_owner[k]
                rel = lax.rem(x - lax.div(owner, CORES) + nx, nx)
                v = u1r[rel, tab_seat[k]]
                keep = lax.rem(owner, CORES) == c
                u2s[i, b] = jnp.where(keep, v, jnp.zeros_like(v))
        for i in range(1, ny):
            u2_copy(i).start()

        @pl.when(dest_core == c)
        def _():
            u2r[c, y_in] = u2s[0]

        @pl.when(dest_core != c)
        def _():
            u2_copy(0).start()

    def s1_copy(hr, i):
        return rcopy(
            s1s.at[hr, i], s1r.at[hr, i], s1ss.at[hr], s1rs.at[hr],
            dev(0, i, c if hr == 0 else oc),
        )

    def shrink_first():
        load_dn.wait()
        for q in range(SEATS):
            k = seat_blk[q]
            a = lax.div(k, per_dev)
            piece = lax.rem(k, per_dev)
            off = lax.rem(lax.div(a, CORES) - x + nx, nx)
            dist = jnp.minimum(off, nx - off)
            ca = lax.rem(a, CORES)
            n_sub = S // per_dev
            rows = [
                tok[piece * n_sub + i + LX * dist, off, ca] for i in range(n_sub)
            ]
            rows = jnp.concatenate(rows, axis=0) if n_sub > 1 else rows[0]
            weight = dn[tab_row[k]]
            v = lax.dot_general(
                weight, rows, (((1,), (1,)), ((), ())),
                preferred_element_type=jnp.float32,
            )
            pos = lax.broadcasted_iota(jnp.int32, v.shape, 1)
            shq[q] = jnp.where(pos < live[k], v, 0.0).astype(shq.dtype)
        for i in range(ny):
            row = lax.rem(y + i, ny)
            for hr in range(CORES):
                h = c if hr == 0 else oc
                for b in range(per_dev):
                    k = row * per_row + h * per_dev + b
                    v = shq[tab_seat[k]]
                    v = jnp.where(tab_owner[k] == ad, v, jnp.zeros_like(v))
                    if hr == 0 and i == 0:
                        s1r[0, 0, b] = v
                    else:
                        s1s[hr, i, b] = v
        for i in range(ny):
            for hr in range(CORES):
                if hr or i:
                    s1_copy(hr, i).start()

    def s2_copy(hr, i):
        return rcopy(
            s2s, s2r.at[hr, i], s2ss.at[hr], s2rs.at[hr],
            dev(i, 0, c if hr == 0 else oc),
        )

    def shrink_second():
        for hr in range(CORES):
            got = s1r.at[hr, pl.ds(1 - hr, ny - 1 + hr)]
            rcopy(got, got, s1ss.at[hr], s1rs.at[hr], dev(0, 0, oc)).wait_recv()
        v = jnp.sum(s1r[...].astype(jnp.float32), axis=(0, 1)).astype(s2s.dtype)
        s2s[...] = v
        s2r[0, 0] = v
        for i in range(nx):
            for hr in range(CORES):
                if hr or i:
                    s2_copy(hr, i).start()

    def chain(o, t):
        d = min(o, ny - o)
        way = 0 if o <= HY else 1
        off = lax.rem(lax.rem(y + o, ny) - x + nx, nx)
        dx = jnp.minimum(off, nx - off)
        s = t - LX * dx - LY * (HY - d) - LAG

        @pl.when((s >= 0) & (s < S))
        def _():
            v = prod.at[s + LX * dx, off]
            top, low = pl.ds(0, R), pl.ds(R, R)
            dt = sb.dtype
            if d == HY:
                sb[0, d - 1, s, top] = v[top].astype(dt)
                sb[1, d - 1, s, top] = v[low].astype(dt)
                y_copy(0, d, s).start()
                y_copy(1, d, s).start()
            elif d == HY - 1:
                add, keep = (top, low) if way == 0 else (low, top)
                sb[way, d - 1, s, keep] = v[keep].astype(dt)
                y_copy(way, d + 1, s).wait_recv()
                got = rb[way, d, s, top].astype(jnp.float32)
                sb[way, d - 1, s, add] = (v[add] + got).astype(dt)
                y_copy(way, d, s).start()
            elif d > 0:
                y_copy(way, d + 1, s).wait_recv()
                got = rb[way, d, s].astype(jnp.float32)
                sb[way, d - 1, s] = (v[...] + got).astype(dt)
                y_copy(way, d, s).start()
            else:
                both = rb.at[:, 0, s]
                rcopy(both, both, ys.at[0, 0], yr.at[0, s], dev(0, 1)).wait_recv()
                total = (
                    v[...]
                    + rb[0, 0, s].astype(jnp.float32)
                    + rb[1, 0, s].astype(jnp.float32)
                )
                fin[0, s] = total[:R]
                fin[1, s] = total[R:]

    def forward(d, t):
        s = t - LX * d

        @pl.when((s >= 0) & (s < S))
        def _():
            both = tok.at[t, pl.ds(0, 1 if d == HX else 2), c]
            rcopy(both, both, xs.at[0, 0], xr.at[d - 1, s], dev(1)).wait_recv()
            if d < HX:
                for way in range(2):
                    x_copy(way, d, s).start()

    def tick(t, carry):
        @pl.when(t == NT + SH2)
        def _():
            shrink_second()

        for k in range(max(HX, HY)):
            if k < HX:
                forward(HX - k, t)
            if k < HY:
                for o in sorted({HY - k, ny - HY + k}):
                    chain(o, t)

        @pl.when(t + AHEAD < S)
        def _():
            own_send(t + AHEAD)

        chain(0, t)

        @pl.when(t < NT)
        def _():
            core_copy(t, c).start()

        @pl.when((t >= 1) & (t <= NT))
        def _():
            core_copy(t - 1, oc).wait_recv()
            v = jnp.dot(
                tok[t - 1].reshape(nx * CORES * R, Fe), w[...],
                preferred_element_type=jnp.float32,
            )
            prod[t - 1] = v.reshape(nx, CORES * R, N)

        @pl.when(t == UP1)
        def _():
            up_first()

        @pl.when(t == UP2)
        def _():
            up_second()

        @pl.when(t == NT)
        def _():
            shrink_first()

        return carry

    lax.fori_loop(0, NT + LY * HY + LAG, tick, 0)

    for p in range(qpc):
        for cs in range(CORES):
            own = (c == cs) & (y == c * qpc + p)

            @pl.when(jnp.logical_not(own))
            def _(cs=cs, p=p):
                rcopy(
                    u2s.at[0], u2r.at[cs, p], u2ss.at[0], u2rs.at[cs, p], dev(0, 0, oc)
                ).wait_recv()

    for hr in range(CORES):
        got = s2r.at[hr, pl.ds(1 - hr, nx - 1 + hr)]
        rcopy(got, got, s2ss.at[hr], s2rs.at[hr], dev(0, 0, oc)).wait_recv()
    stores = []
    for hr in range(CORES):
        h = c if hr == 0 else oc
        sh = s2r[hr, 0]
        for i in range(1, nx):
            sh = sh + s2r[hr, i]
        n_sub = S // per_dev
        for b in range(per_dev):
            blk = h * per_dev + b
            up = jnp.concatenate(
                [u2r[0, p, blk] + u2r[1, p, blk] for p in range(qpc)], axis=1
            )
            part = lax.dot_general(
                sh[b], up, (((0,), (0,)), ((), ())),
                preferred_element_type=jnp.float32,
            )
            base = fin[h, pl.ds(b * n_sub, n_sub)].reshape(n_sub * R, N)
            start = pl.multiple_of(h * (S * R) + b * BLOCK, BLOCK)
            obuf[hr, b] = (base + adapter_scale * part).astype(out.dtype)
            store = pltpu.make_async_copy(
                obuf.at[hr, b], out.at[pl.ds(start, BLOCK)], st_sem.at[hr, b]
            )
            store.start()
            stores.append(store)

    for store in stores:
        store.wait()

    def sent(ref, sem):
        rcopy(ref, ref, sem, dr.at[0], dev(0, 0, oc)).wait_send()

    for way in range(2):
        sent(tok.at[pl.ds(0, S), pl.ds(0, HX - 1), c], xs.at[way, 0])
        sent(tok.at[pl.ds(0, S), 0, c, :, pl.ds(0, half)], xs.at[way, 1])
        sent(sb.at[way, pl.ds(0, HY - 1)], ys.at[way, 0])
        sent(sb.at[way, HY - 1, :, pl.ds(0, R)], ys.at[way, 1])
    sent(tok.at[:, :, c], ds.at[0])
    sent(u1s.at[pl.ds(1, nx - 1)], u1ss.at[0])
    sent(u2s.at[pl.ds(1, ny - 1)], u2ss.at[1])

    @pl.when(dest_core != c)
    def _():
        u2_copy(0).wait_send()

    for hr in range(CORES):
        sent(s1s.at[hr, pl.ds(1 - hr, ny - 1 + hr)], s1ss.at[hr])
        sent(s2r.at[hr, pl.ds(1 - hr, nx - 1 + hr)], s2ss.at[hr])


def on_device(tokens, query_weight, down, up, ids, live, slots):
    nx = lax.axis_size("adapter") // CORES
    ny = lax.axis_size("tensor")
    rows, Fe = tokens.shape
    N = query_weight.shape[1]
    slots_dev, rank = down.shape[0], down.shape[1]
    R = rows // SUB
    NT = SUB + LX * (nx // 2)
    HX, HY = nx // 2, ny // 2
    lanes = N * CORES // ny
    qpc = N // lanes
    per_row = ids.shape[0] // ny
    per_dev = per_row // CORES
    bf = jnp.bfloat16
    dma = pltpu.SemaphoreType.DMA
    smem = pl.BlockSpec(memory_space=pltpu.SMEM)
    hbm = pl.BlockSpec(memory_space=pl.ANY)
    piece = (per_dev, rank, BLOCK)
    return pl.pallas_call(
        functools.partial(kernel, nx, ny),
        out_shape=jax.ShapeDtypeStruct((CORES * rows, N), bf),
        in_specs=[smem] * 3 + [hbm] * 4,
        out_specs=hbm,
        scratch_shapes=[
            pltpu.VMEM((NT, nx, CORES, R, Fe), bf),
            pltpu.VMEM((Fe, N), bf),
            pltpu.VMEM((slots_dev, rank, Fe), bf),
            pltpu.VMEM((nx, slots_dev, rank, lanes), bf),
            pltpu.VMEM((NT, nx, CORES * R, N), jnp.float32),
            pltpu.VMEM((2, HY, SUB, CORES * R, N), bf),
            pltpu.VMEM((2, HY, SUB, CORES * R, N), bf),
            pltpu.VMEM((CORES, SUB, R, N), jnp.float32),
            pltpu.VMEM((nx, SEATS, rank, lanes), bf),
            pltpu.VMEM((nx, SEATS, rank, lanes), bf),
            pltpu.VMEM((ny, per_row, rank, lanes), bf),
            pltpu.VMEM((CORES, qpc, per_row, rank, lanes), bf),
            pltpu.VMEM((SEATS, rank, BLOCK), bf),
            pltpu.VMEM((CORES, ny) + piece, bf),
            pltpu.VMEM((CORES, ny) + piece, bf),
            pltpu.VMEM(piece, bf),
            pltpu.VMEM((CORES, nx) + piece, bf),
            pltpu.SMEM((ids.shape[0],), jnp.int32),
            pltpu.SMEM((ids.shape[0],), jnp.int32),
            pltpu.SMEM((ids.shape[0],), jnp.int32),
            pltpu.VMEM((CORES, per_dev, BLOCK, N), bf),
            dma((CORES, per_dev)),
            dma((4,)),
            dma((2, 2)), dma((HX, SUB)),
            dma((1,)), dma((NT,)),
            dma((2, 2)), dma((2 * HY - 1, SUB)),
            dma((1,)), dma((1,)),
            dma((2,)), dma((CORES, qpc)),
            dma((CORES,)), dma((CORES,)),
            dma((CORES,)), dma((CORES,)),
        ],
        compiler_params=pltpu.CompilerParams(
            collective_id=0, has_side_effects=True,
            vmem_limit_bytes=60 * 1024 * 1024,
        ),
    )(ids, live, slots, tokens.reshape(SUB, R, Fe), query_weight, down, up)


def solution(mesh):
    placed = (
        P(("groups", "adapter"), "tensor"),
        P("tensor", "adapter"),
        P("adapter", None, "tensor"),
        P("adapter", None, None),
        P("groups"),
        P("groups"),
        P("groups"),
    )
    return jax.shard_map(
        on_device,
        mesh=mesh,
        in_specs=placed,
        out_specs=P(("groups", "tensor"), "adapter"),
        check_vma=False,
    )
```

```python
import functools

import jax
import jax.numpy as jnp
from jax import lax
from jax.experimental import pallas as pl
from jax.experimental.pallas import tpu as pltpu
from jax.sharding import PartitionSpec as P

MESH = pl.DeviceIdType.MESH
BLOCK = 128
CORES = 2
SUB = 16
LX = 2
LY = 2
LAG = 2
AHEAD = 2
SEATS = 4
UP1 = 1
UP2 = 6
SH2 = 3
adapter_scale = 2.0


def kernel(
    nx, ny,
    ids, live, slots, tok_h, w_h, dn_h, up_h,
    out,
    tok, w, dn, upv, prod, sb, rb, fin,
    u1s, u1r, u2s, u2r, shq, s1s, s1r, s2s, s2r,
    tab_owner, tab_row, tab_seat,
    obuf, st_sem, ld_sem, xs, xr, ds, dr, ys, yr,
    u1ss, u1rs, u2ss, u2rs, s1ss, s1rs, s2ss, s2rs,
):
    S = SUB
    R, Fe = tok.shape[3], tok.shape[4]
    half = Fe // 2
    N = w.shape[1]
    slots_dev = dn.shape[0]
    HX, HY = nx // 2, ny // 2
    NT = tok.shape[0]
    nblk = ids.shape[0]
    per_row = nblk // ny
    per_dev = per_row // CORES
    lanes = upv.shape[3]
    qpc = N // lanes

    ad = lax.axis_index("adapter")
    y = lax.axis_index("tensor")
    x = lax.div(ad, CORES)
    c = lax.rem(ad, CORES)
    oc = 1 - c

    def dev(dx=0, dy=0, core=None):
        core = c if core is None else core
        return {
            "adapter": lax.rem(x + (dx + nx) % nx, nx) * CORES + core,
            "tensor": lax.rem(y + (dy + ny) % ny, ny),
        }

    def rcopy(src, dst, ssem, rsem, where):
        return pltpu.make_async_remote_copy(
            src_ref=src, dst_ref=dst, send_sem=ssem, recv_sem=rsem,
            device_id=where, device_id_type=MESH,
        )

    load_tok = pltpu.make_async_copy(tok_h, tok.at[pl.ds(0, S), 0, c], ld_sem.at[0])

    def load_up(i):
        return pltpu.make_async_copy(
            up_h.at[:, :, pl.ds(pl.multiple_of(i * N * CORES + y * lanes, lanes), lanes)],
            upv.at[i], ld_sem.at[3],
        )

    load_w = pltpu.make_async_copy(w_h, w, ld_sem.at[1])
    load_dn = pltpu.make_async_copy(dn_h, dn, ld_sem.at[2])
    load_tok.start()
    load_w.start()
    load_dn.start()
    for i in range(nx):
        load_up(i).start()

    barrier = pltpu.get_barrier_semaphore()
    peers = [(i, 0) for i in range(nx)] + [(0, i) for i in range(1, ny)]
    for px, py in peers:
        for core in (c, oc):
            if px or py or core is oc:
                pl.semaphore_signal(
                    barrier, inc=1, device_id=dev(px, py, core), device_id_type=MESH
                )
    pl.semaphore_wait(barrier, CORES * len(peers) - 1)

    def x_copy(way, d, s):
        off = (nx - d) % nx if way == 0 else d
        noff = nx - d - 1 if way == 0 else d + 1
        t = s + LX * d
        src = tok.at[t, off, c]
        dst = tok.at[t + LX, noff, c]
        if d == HX - 1:
            cols = pl.ds(way * half, half)
            src, dst = src.at[:, cols], dst.at[:, cols]
        return rcopy(
            src, dst, xs.at[way, 1 if d == HX - 1 else 0], xr.at[d, s],
            dev(1 if way == 0 else -1),
        )

    def core_copy(t, core):
        part = tok.at[t, :, core]
        return rcopy(part, part, ds.at[0], dr.at[t], dev(0, 0, oc))

    def own_send(s):
        x_copy(0, 0, s).start()
        x_copy(1, 0, s).start()

    def y_copy(way, d, s):
        src, dst = sb.at[way, d - 1, s], rb.at[way, d - 1, s]
        if d == HY:
            src, dst = src.at[pl.ds(0, R)], dst.at[pl.ds(0, R)]
        return rcopy(
            src, dst, ys.at[way, 1 if d == HY else 0],
            yr.at[0 if d == 1 else d - 1 + way * (HY - 1), s],
            dev(0, 1 if way == 0 else -1),
        )

    load_tok.wait()
    for s in range(AHEAD):
        own_send(s)

    def place(k, carry):
        slot = slots[ids[k]]
        tab_owner[k] = lax.div(slot, slots_dev)
        tab_row[k] = lax.rem(slot, slots_dev)
        return carry

    lax.fori_loop(0, nblk, place, 0)

    def plan(k, seats):
        owner = tab_owner[k]
        seat = jnp.int32(0)
        for i in range(nblk):
            seat += jnp.where((tab_owner[i] == owner) & (i < k), 1, 0)
        seat = jnp.minimum(seat, SEATS - 1)
        tab_seat[k] = seat
        mine = owner == ad
        return tuple(
            jnp.where(mine & (seat == q), k, seats[q]) for q in range(SEATS)
        )

    seat_blk = lax.fori_loop(0, nblk, plan, (jnp.int32(0),) * SEATS)

    load_w.wait()

    def u1_copy(i):
        return rcopy(u1s.at[i], u1r.at[i], u1ss.at[0], u1rs.at[0], dev(i))

    def up_first():
        pltpu.make_async_copy(upv, upv, ld_sem.at[3]).wait()
        for q in range(SEATS):
            row = tab_row[seat_blk[q]]
            for i in range(nx):
                v = upv[lax.rem(x + i, nx), row]
                if i == 0:
                    u1r[0, q] = v
                else:
                    u1s[i, q] = v
        for i in range(1, nx):
            u1_copy(i).start()

    dest_core = lax.div(y, qpc)
    y_in = lax.rem(y, qpc)

    def u2_copy(i):
        return rcopy(
            u2s.at[i], u2r.at[c, y_in], u2ss.at[min(i, 1)], u2rs.at[c, y_in],
            dev(0, i, dest_core),
        )

    def up_second():
        rest = u1r.at[pl.ds(1, nx - 1)]
        rcopy(rest, rest, u1ss.at[0], u1rs.at[0], dev(1)).wait_recv()
        for i in range(ny):
            row = lax.rem(y + i, ny)
            for b in range(per_row):
                k = row * per_row + b
                owner = tab_owner[k]
                rel = lax.rem(x - lax.div(owner, CORES) + nx, nx)
                v = u1r[rel, tab_seat[k]]
                keep = lax.rem(owner, CORES) == c
                u2s[i, b] = jnp.where(keep, v, jnp.zeros_like(v))
        for i in range(1, ny):
            u2_copy(i).start()

        @pl.when(dest_core == c)
        def _():
            u2r[c, y_in] = u2s[0]

        @pl.when(dest_core != c)
        def _():
            u2_copy(0).start()

    def s1_copy(hr, i):
        return rcopy(
            s1s.at[hr, i], s1r.at[hr, i], s1ss.at[hr], s1rs.at[hr],
            dev(0, i, c if hr == 0 else oc),
        )

    def shrink_first():
        load_dn.wait()
        for q in range(SEATS):
            k = seat_blk[q]
            a = lax.div(k, per_dev)
            piece = lax.rem(k, per_dev)
            off = lax.rem(lax.div(a, CORES) - x + nx, nx)
            dist = jnp.minimum(off, nx - off)
            ca = lax.rem(a, CORES)
            n_sub = S // per_dev
            rows = [
                tok[piece * n_sub + i + LX * dist, off, ca] for i in range(n_sub)
            ]
            rows = jnp.concatenate(rows, axis=0) if n_sub > 1 else rows[0]
            weight = dn[tab_row[k]]
            v = lax.dot_general(
                weight, rows, (((1,), (1,)), ((), ())),
                preferred_element_type=jnp.float32,
            )
            pos = lax.broadcasted_iota(jnp.int32, v.shape, 1)
            shq[q] = jnp.where(pos < live[k], v, 0.0).astype(shq.dtype)
        for i in range(ny):
            row = lax.rem(y + i, ny)
            for hr in range(CORES):
                h = c if hr == 0 else oc
                for b in range(per_dev):
                    k = row * per_row + h * per_dev + b
                    v = shq[tab_seat[k]]
                    v = jnp.where(tab_owner[k] == ad, v, jnp.zeros_like(v))
                    if hr == 0 and i == 0:
                        s1r[0, 0, b] = v
                    else:
                        s1s[hr, i, b] = v
        for i in range(ny):
            for hr in range(CORES):
                if hr or i:
                    s1_copy(hr, i).start()

    def s2_copy(hr, i):
        return rcopy(
            s2s, s2r.at[hr, i], s2ss.at[hr], s2rs.at[hr],
            dev(i, 0, c if hr == 0 else oc),
        )

    def shrink_second():
        for hr in range(CORES):
            got = s1r.at[hr, pl.ds(1 - hr, ny - 1 + hr)]
            rcopy(got, got, s1ss.at[hr], s1rs.at[hr], dev(0, 0, oc)).wait_recv()
        v = jnp.sum(s1r[...].astype(jnp.float32), axis=(0, 1)).astype(s2s.dtype)
        s2s[...] = v
        s2r[0, 0] = v
        for i in range(nx):
            for hr in range(CORES):
                if hr or i:
                    s2_copy(hr, i).start()

    def chain(o, t):
        d = min(o, ny - o)
        way = 0 if o <= HY else 1
        off = lax.rem(lax.rem(y + o, ny) - x + nx, nx)
        dx = jnp.minimum(off, nx - off)
        s = t - LX * dx - LY * (HY - d) - LAG

        @pl.when((s >= 0) & (s < S))
        def _():
            v = prod.at[s + LX * dx, off]
            top, low = pl.ds(0, R), pl.ds(R, R)
            dt = sb.dtype
            if d == HY:
                sb[0, d - 1, s, top] = v[top].astype(dt)
                sb[1, d - 1, s, top] = v[low].astype(dt)
                y_copy(0, d, s).start()
                y_copy(1, d, s).start()
            elif d == HY - 1:
                add, keep = (top, low) if way == 0 else (low, top)
                sb[way, d - 1, s, keep] = v[keep].astype(dt)
                y_copy(way, d + 1, s).wait_recv()
                got = rb[way, d, s, top].astype(jnp.float32)
                sb[way, d - 1, s, add] = (v[add] + got).astype(dt)
                y_copy(way, d, s).start()
            elif d > 0:
                y_copy(way, d + 1, s).wait_recv()
                got = rb[way, d, s].astype(jnp.float32)
                sb[way, d - 1, s] = (v[...] + got).astype(dt)
                y_copy(way, d, s).start()
            else:
                both = rb.at[:, 0, s]
                rcopy(both, both, ys.at[0, 0], yr.at[0, s], dev(0, 1)).wait_recv()
                total = (
                    v[...]
                    + rb[0, 0, s].astype(jnp.float32)
                    + rb[1, 0, s].astype(jnp.float32)
                )
                fin[0, s] = total[:R]
                fin[1, s] = total[R:]

    def forward(d, t):
        s = t - LX * d

        @pl.when((s >= 0) & (s < S))
        def _():
            both = tok.at[t, pl.ds(0, 1 if d == HX else 2), c]
            rcopy(both, both, xs.at[0, 0], xr.at[d - 1, s], dev(1)).wait_recv()
            if d < HX:
                for way in range(2):
                    x_copy(way, d, s).start()

    def tick(t, carry):
        @pl.when(t == NT + SH2)
        def _():
            shrink_second()

        for k in range(max(HX, HY)):
            if k < HX:
                forward(HX - k, t)
            if k < HY:
                for o in sorted({HY - k, ny - HY + k}):
                    chain(o, t)

        @pl.when(t + AHEAD < S)
        def _():
            own_send(t + AHEAD)

        chain(0, t)

        @pl.when(t < NT)
        def _():
            core_copy(t, c).start()

        @pl.when((t >= 1) & (t <= NT))
        def _():
            core_copy(t - 1, oc).wait_recv()
            v = jnp.dot(
                tok[t - 1].reshape(nx * CORES * R, Fe), w[...],
                preferred_element_type=jnp.float32,
            )
            prod[t - 1] = v.reshape(nx, CORES * R, N)

        @pl.when(t == UP1)
        def _():
            up_first()

        @pl.when(t == UP2)
        def _():
            up_second()

        @pl.when(t == NT)
        def _():
            shrink_first()

        return carry

    lax.fori_loop(0, NT + LY * HY + LAG, tick, 0)

    for p in range(qpc):
        for cs in range(CORES):
            own = (c == cs) & (y == c * qpc + p)

            @pl.when(jnp.logical_not(own))
            def _(cs=cs, p=p):
                rcopy(
                    u2s.at[0], u2r.at[cs, p], u2ss.at[0], u2rs.at[cs, p], dev(0, 0, oc)
                ).wait_recv()

    for hr in range(CORES):
        got = s2r.at[hr, pl.ds(1 - hr, nx - 1 + hr)]
        rcopy(got, got, s2ss.at[hr], s2rs.at[hr], dev(0, 0, oc)).wait_recv()
    stores = []
    for hr in range(CORES):
        h = c if hr == 0 else oc
        sh = s2r[hr, 0]
        for i in range(1, nx):
            sh = sh + s2r[hr, i]
        n_sub = S // per_dev
        for b in range(per_dev):
            blk = h * per_dev + b
            up = jnp.concatenate(
                [u2r[0, p, blk] + u2r[1, p, blk] for p in range(qpc)], axis=1
            )
            part = lax.dot_general(
                sh[b], up, (((0,), (0,)), ((), ())),
                preferred_element_type=jnp.float32,
            )
            base = fin[h, pl.ds(b * n_sub, n_sub)].reshape(n_sub * R, N)
            start = pl.multiple_of(h * (S * R) + b * BLOCK, BLOCK)
            obuf[hr, b] = (base + adapter_scale * part).astype(out.dtype)
            store = pltpu.make_async_copy(
                obuf.at[hr, b], out.at[pl.ds(start, BLOCK)], st_sem.at[hr, b]
            )
            store.start()
            stores.append(store)

    for store in stores:
        store.wait()

    def sent(ref, sem):
        rcopy(ref, ref, sem, dr.at[0], dev(0, 0, oc)).wait_send()

    for way in range(2):
        sent(tok.at[pl.ds(0, S), pl.ds(0, HX - 1), c], xs.at[way, 0])
        sent(tok.at[pl.ds(0, S), 0, c, :, pl.ds(0, half)], xs.at[way, 1])
        sent(sb.at[way, pl.ds(0, HY - 1)], ys.at[way, 0])
        sent(sb.at[way, HY - 1, :, pl.ds(0, R)], ys.at[way, 1])
    sent(tok.at[:, :, c], ds.at[0])
    sent(u1s.at[pl.ds(1, nx - 1)], u1ss.at[0])
    sent(u2s.at[pl.ds(1, ny - 1)], u2ss.at[1])

    @pl.when(dest_core != c)
    def _():
        u2_copy(0).wait_send()

    for hr in range(CORES):
        sent(s1s.at[hr, pl.ds(1 - hr, ny - 1 + hr)], s1ss.at[hr])
        sent(s2r.at[hr, pl.ds(1 - hr, nx - 1 + hr)], s2ss.at[hr])


def on_device(tokens, query_weight, down, up, ids, live, slots):
    nx = lax.axis_size("adapter") // CORES
    ny = lax.axis_size("tensor")
    rows, Fe = tokens.shape
    N = query_weight.shape[1]
    slots_dev, rank = down.shape[0], down.shape[1]
    R = rows // SUB
    NT = SUB + LX * (nx // 2)
    HX, HY = nx // 2, ny // 2
    lanes = N * CORES // ny
    qpc = N // lanes
    per_row = ids.shape[0] // ny
    per_dev = per_row // CORES
    bf = jnp.bfloat16
    dma = pltpu.SemaphoreType.DMA
    smem = pl.BlockSpec(memory_space=pltpu.SMEM)
    hbm = pl.BlockSpec(memory_space=pl.ANY)
    piece = (per_dev, rank, BLOCK)
    return pl.pallas_call(
        functools.partial(kernel, nx, ny),
        out_shape=jax.ShapeDtypeStruct((CORES * rows, N), bf),
        in_specs=[smem] * 3 + [hbm] * 4,
        out_specs=hbm,
        scratch_shapes=[
            pltpu.VMEM((NT, nx, CORES, R, Fe), bf),
            pltpu.VMEM((Fe, N), bf),
            pltpu.VMEM((slots_dev, rank, Fe), bf),
            pltpu.VMEM((nx, slots_dev, rank, lanes), bf),
            pltpu.VMEM((NT, nx, CORES * R, N), jnp.float32),
            pltpu.VMEM((2, HY, SUB, CORES * R, N), bf),
            pltpu.VMEM((2, HY, SUB, CORES * R, N), bf),
            pltpu.VMEM((CORES, SUB, R, N), jnp.float32),
            pltpu.VMEM((nx, SEATS, rank, lanes), bf),
            pltpu.VMEM((nx, SEATS, rank, lanes), bf),
            pltpu.VMEM((ny, per_row, rank, lanes), bf),
            pltpu.VMEM((CORES, qpc, per_row, rank, lanes), bf),
            pltpu.VMEM((SEATS, rank, BLOCK), bf),
            pltpu.VMEM((CORES, ny) + piece, bf),
            pltpu.VMEM((CORES, ny) + piece, bf),
            pltpu.VMEM(piece, bf),
            pltpu.VMEM((CORES, nx) + piece, bf),
            pltpu.SMEM((ids.shape[0],), jnp.int32),
            pltpu.SMEM((ids.shape[0],), jnp.int32),
            pltpu.SMEM((ids.shape[0],), jnp.int32),
            pltpu.VMEM((CORES, per_dev, BLOCK, N), bf),
            dma((CORES, per_dev)),
            dma((4,)),
            dma((2, 2)), dma((HX, SUB)),
            dma((1,)), dma((NT,)),
            dma((2, 2)), dma((2 * HY - 1, SUB)),
            dma((1,)), dma((1,)),
            dma((2,)), dma((CORES, qpc)),
            dma((CORES,)), dma((CORES,)),
            dma((CORES,)), dma((CORES,)),
        ],
        compiler_params=pltpu.CompilerParams(
            collective_id=0, has_side_effects=True,
            vmem_limit_bytes=60 * 1024 * 1024,
        ),
    )(ids, live, slots, tokens.reshape(SUB, R, Fe), query_weight, down, up)


def solution(mesh):
    placed = (
        P(("groups", "adapter"), "tensor"),
        P("tensor", "adapter"),
        P("adapter", None, "tensor"),
        P("adapter", None, None),
        P("groups"),
        P("groups"),
        P("groups"),
    )
    return jax.shard_map(
        on_device,
        mesh=mesh,
        in_specs=placed,
        out_specs=P(("groups", "tensor"), "adapter"),
        check_vma=False,
    )
```
